16 devices in a mesh: dp: 4 (over z, y), sp: 4 (over x, core).
Axes of the slice: x: 2, y: 2, z: 2, core: 2. Of those that a mesh axis runs over, the one named last changes fastest.
Arguments:
- tokens: bfloat16 [32768, 384], P(('dp', 'sp')), parts along dimension 0
- grad_out: bfloat16 [32768, 384], P(('dp', 'sp')), parts along dimension 0
- ln_gain: float32 [384], replicated
- ln_bias: float32 [384], replicated
- w_qkv: bfloat16 [384, 1152], replicated
- w_out: bfloat16 [384, 384], replicated
- temperature: float32 [8], replicated
Outputs:
- output 1: bfloat16 [32768, 384], P(('dp', 'sp')), parts along dimension 0
- output 2: bfloat16 [32768, 384], P(('dp', 'sp')), parts along dimension 0
- output 3: float32 [1536, 1152], P(('dp', 'sp')), parts along dimension 0
- output 4: float32 [1536, 384], P(('dp', 'sp')), parts along dimension 0
- output 5: float32 [1536], P('dp'), parts along dimension 0
- output 6: float32 [1536], P('dp'), parts along dimension 0
- output 7: float32 [32], P('dp'), parts along dimension 0
There are 4 independent parts. The reference program is written for one: setup_inputs(seed, part) draws one part's arguments, and reference() takes and returns one part's arrays. A program takes and returns all parts, laid end to end along the dimension named above; an argument that names none is the same for every part.
All inputs are finite; a program needn't handle non-finite values.
Results may differ from the reference program's by a relative error of at most 0.00130225.
Values are sent between devices in bfloat16 or wider.
A program may use at most 1 GiB of HBM per device.

```python
import jax
import jax.numpy as jnp
from jax import lax

SEQ_LEN = 8192
MODEL_DIM = 384
NUM_HEADS = 8

HEAD_DIM = MODEL_DIM // NUM_HEADS


def setup_inputs(seed: int = 0, part: int = 0) -> dict:
    part_keys = jax.random.split(jax.random.fold_in(jax.random.key(seed), part), 4)
    shared_keys = jax.random.split(jax.random.key(seed + 1), 5)
    position = (jnp.arange(SEQ_LEN, dtype=jnp.float32) + 0.5) / SEQ_LEN
    wave_basis = jnp.cos(jnp.pi * position[:, None] * jnp.arange(1, 5, dtype=jnp.float32)[None, :])
    x_pattern = jnp.dot(wave_basis, jax.random.normal(part_keys[0], (4, MODEL_DIM), jnp.float32))
    tokens = jax.random.normal(part_keys[1], (SEQ_LEN, MODEL_DIM), jnp.float32) + x_pattern
    dy_pattern = jnp.dot(wave_basis, jax.random.normal(part_keys[2], (4, MODEL_DIM), jnp.float32))
    grad_out = jax.random.normal(part_keys[3], (SEQ_LEN, MODEL_DIM), jnp.float32) + 0.5 * dy_pattern
    w_scale = MODEL_DIM ** -0.5
    return {
        'tokens': tokens.astype(jnp.bfloat16),
        'grad_out': grad_out.astype(jnp.bfloat16),
        'ln_gain': 1.0 + 0.3 * jax.random.normal(shared_keys[0], (MODEL_DIM,), jnp.float32),
        'ln_bias': 0.3 * jax.random.normal(shared_keys[1], (MODEL_DIM,), jnp.float32),
        'w_qkv': (w_scale * jax.random.normal(shared_keys[2], (MODEL_DIM, 3 * MODEL_DIM), jnp.float32)).astype(jnp.bfloat16),
        'w_out': (w_scale * jax.random.normal(shared_keys[3], (MODEL_DIM, MODEL_DIM), jnp.float32)).astype(jnp.bfloat16),
        'temperature': jax.random.uniform(shared_keys[4], (NUM_HEADS,), jnp.float32, 2.5, 6.5),
    }


def layer_norm(x_f32, ln_gain, ln_bias):
    row_mean = jnp.mean(x_f32, axis=-1, keepdims=True)
    centered = x_f32 - row_mean
    row_var = jnp.mean(centered * centered, axis=-1, keepdims=True)
    return centered * lax.rsqrt(row_var + 1e-6) * ln_gain + ln_bias


def attn_probs(gram_sum, q_sq, k_sq, temperature):
    cosine = gram_sum / (jnp.sqrt(q_sq)[..., :, None] * jnp.sqrt(k_sq)[..., None, :])
    return jax.nn.softmax(temperature[..., None, None] * cosine, axis=-1)


def reference(tokens, grad_out, ln_gain, ln_bias, w_qkv, w_out, temperature):
    x_f32 = tokens.astype(jnp.float32)
    ln_value, ln_vjp = jax.vjp(layer_norm, x_f32, ln_gain, ln_bias)
    normed = ln_value.astype(jnp.bfloat16)
    qkv_act = jnp.dot(normed, w_qkv, preferred_element_type=jnp.float32).astype(jnp.bfloat16)
    qkv_heads = qkv_act.astype(jnp.float32).reshape(SEQ_LEN, 3, NUM_HEADS, HEAD_DIM)
    q_heads = qkv_heads[:, 0]
    k_heads = qkv_heads[:, 1]
    v_heads = qkv_heads[:, 2]
    gram_sum = jnp.einsum('nhi,nhj->hij', q_heads, k_heads)
    q_sq = jnp.sum(q_heads * q_heads, axis=0)
    k_sq = jnp.sum(k_heads * k_heads, axis=0)
    attn_f32, probs_vjp = jax.vjp(attn_probs, gram_sum, q_sq, k_sq, temperature)
    attn_weights = attn_f32.astype(jnp.bfloat16).astype(jnp.float32)
    attn_out = jnp.einsum('nhj,hij->nhi', v_heads, attn_weights).astype(jnp.bfloat16).reshape(SEQ_LEN, MODEL_DIM)
    out_tokens = (x_f32 + jnp.dot(attn_out, w_out, preferred_element_type=jnp.float32)).astype(jnp.bfloat16)

    grad_w_out = jnp.dot(attn_out.T, grad_out, preferred_element_type=jnp.float32)
    d_attn = jnp.dot(grad_out, w_out.T, preferred_element_type=jnp.float32).astype(jnp.bfloat16)
    d_heads = d_attn.astype(jnp.float32).reshape(SEQ_LEN, NUM_HEADS, HEAD_DIM)
    d_probs = jnp.einsum('nhi,nhj->hij', d_heads, v_heads)
    d_gram, d_qsq, d_ksq, grad_temperature = probs_vjp(d_probs)
    d_gram_bf = d_gram.astype(jnp.bfloat16).astype(jnp.float32)
    d_q = jnp.einsum('hij,nhj->nhi', d_gram_bf, k_heads) + 2.0 * q_heads * d_qsq
    d_k = jnp.einsum('hij,nhi->nhj', d_gram_bf, q_heads) + 2.0 * k_heads * d_ksq
    d_v = jnp.einsum('hij,nhi->nhj', attn_weights, d_heads)
    d_qkv = jnp.stack([d_q, d_k, d_v], axis=1).astype(jnp.bfloat16).reshape(SEQ_LEN, 3 * MODEL_DIM)
    grad_w_qkv = jnp.dot(normed.T, d_qkv, preferred_element_type=jnp.float32)
    d_normed = jnp.dot(d_qkv, w_qkv.T, preferred_element_type=jnp.float32)
    d_x, grad_gain, grad_bias = ln_vjp(d_normed)
    grad_tokens = (grad_out.astype(jnp.float32) + d_x).astype(jnp.bfloat16)
    return (out_tokens, grad_tokens, grad_w_qkv, grad_w_out, grad_gain, grad_bias, grad_temperature)
```

```python
import jax
import jax.numpy as jnp
from jax import lax
from jax.experimental import pallas as pl
from jax.experimental.pallas import tpu as pltpu
from jax.sharding import PartitionSpec as P

F32 = jnp.float32
BF16 = jnp.bfloat16
MESH = pl.DeviceIdType.MESH
C = 384
GC = 192
HD = 48
NT = 2048
BLK = 256
NB = NT // BLK
EPS = 1e-6

S_GRAM, S_DPROB, S_ATTN, S_DGRAM, S_DSQ = 0, 3, 6, 7, 8
S_GWO, S_GWV, S_GWQK, S_LN = 9, 12, 15, 18
N_SEM = 21


def nn(a, b):
    return jnp.dot(a, b, preferred_element_type=F32)


def nt(a, b):
    return lax.dot_general(a, b, (((1,), (1,)), ((), ())), preferred_element_type=F32)


def transpose_bf16(a):
    return a.T


def lanes(shape):
    return lax.broadcasted_iota(jnp.int32, shape, len(shape) - 1)


def rows(shape):
    return lax.broadcasted_iota(jnp.int32, shape, 0)


def pack_heads(dense_ref, dst_ref, g, sq_col=None, sk_col=None):
    lane = lanes((HD, 128))
    for pair in range(2):
        total = jnp.zeros((HD, 128), F32)
        for side in range(2):
            h = 2 * pair + side
            r = pl.ds(HD * h, HD)
            block = dense_ref[g, r, :]
            block = pltpu.roll(block, (64 * side - HD * h) % 256, 1)[:, :128]
            base = 64 * side
            total = jnp.where((lane >= base) & (lane < base + HD), block, total)
            if sq_col is not None:
                rr = slice(HD * h, HD * h + HD)
                total = jnp.where(lane == base + HD, sq_col[rr], total)
                total = jnp.where(lane == base + HD + 1, sk_col[rr], total)
        dst_ref[g, pl.ds(HD * pair, HD), :] = total


def unpack_heads(packed):
    parts = []
    for pair in range(2):
        p = packed[HD * pair:HD * pair + HD]
        parts += [p, pltpu.roll(p, 64, 1)]
    return jnp.concatenate(parts, axis=0)


def spread_heads(compact):
    parts = []
    for h in range(4):
        block = compact[HD * h:HD * h + HD]
        block = jnp.concatenate([block, jnp.zeros((HD, 128), F32)], axis=1)
        parts.append(pltpu.roll(block, HD * h, 1) if h else block)
    return jnp.concatenate(parts, axis=0)


def col(x, lane, index):
    return jnp.sum(jnp.where(lane == index, x, 0.0), axis=1, keepdims=True)


def per_head_row(column):
    parts = []
    for h in range(4):
        part = jnp.broadcast_to(column[HD * h:HD * h + HD], (HD, 128))
        eye = rows((HD, 128)) == lanes((HD, 128))
        row = jnp.sum(jnp.where(eye, part, 0.0), axis=0, keepdims=True)
        parts.append(jnp.broadcast_to(row, (HD, 128)))
    return jnp.concatenate(parts, axis=0)


def per_head_sum_col(x):
    parts = []
    for h in range(4):
        row = jnp.sum(x[HD * h:HD * h + HD], axis=0, keepdims=True)
        eye = rows((HD, 128)) == lanes((HD, 128))
        parts.append(jnp.sum(jnp.where(eye, jnp.broadcast_to(row, (HD, 128)), 0.0), axis=1, keepdims=True))
    return jnp.concatenate(parts, axis=0)


def body(x_hbm, dy_hbm, gain_ref, bias_ref, wqkv_hbm, wout_hbm, temp_ref,
         out_hbm, gt_hbm, gwqkv_hbm, gwout_hbm, gg_ref, gb_ref, gtemp_ref,
         x_v, dy_v, w_v, wo_v, wT, woT, xT, dyT, uT, mean_v, rstd_v, qkvT, doT, oT, dqkvT, outR, gtR,
         gainB, biasB, ssq, gacc, dacc, gsend, grecv, dsend, drecv, lhsA, lhsAT, lhsD, lhsDT, dsq_v,
         Po, Pv, Pqk, Ro, Rv, Rqk, To, Tv, Tqk, Io, Iv, Iqk, lnsend, lnrecv, lnacc,
         ssem, rsem, dsem):
    s = lax.axis_index("sp")
    chip, core = s // 2, s % 2
    sib = chip * 2 + (1 - core)
    cp = (1 - chip) * 2 + core
    dg = (1 - chip) * 2 + (1 - core)
    other = 1 - core

    barrier = pltpu.get_barrier_semaphore()
    for dev in (sib, cp, dg):
        pl.semaphore_signal(barrier, inc=1, device_id={"sp": dev}, device_id_type=MESH)

    def remote(src, dst, i, dev):
        return pltpu.make_async_remote_copy(src_ref=src, dst_ref=dst, send_sem=ssem.at[i], recv_sem=rsem.at[i],
                                            device_id={"sp": dev}, device_id_type=MESH)

    def local(src, dst, i):
        return pltpu.make_async_copy(src, dst, dsem.at[i])

    nx = 4
    xr = NT // nx
    in_w = local(wqkv_hbm, w_v, 0)
    in_wo = local(wout_hbm, wo_v, 1)
    in_x = [local(x_hbm.at[pl.ds(i * xr, xr)], x_v.at[pl.ds(i * xr, xr)], 2 + i) for i in range(nx)]
    in_dy = [local(dy_hbm.at[pl.ds(i * xr, xr)], dy_v.at[pl.ds(i * xr, xr)], 6 + i) for i in range(nx)]
    in_x[0].start()
    in_w.start()
    for d in in_x[1:] + [in_wo] + in_dy:
        d.start()

    gainB[...] = jnp.broadcast_to(gain_ref[...], (128, C)).T
    biasB[...] = jnp.broadcast_to(bias_ref[...], (128, C)).T
    gacc[...] = jnp.zeros(gacc.shape, F32)
    dacc[...] = jnp.zeros(dacc.shape, F32)

    def wide(ref):
        v = ref[...]
        return jnp.concatenate([v] * (BLK // 128), axis=1)

    for b in range(NB):
        t = pl.ds(b * BLK, BLK)
        if (b * BLK) % xr == 0:
            in_x[b * BLK // xr].wait()
        xt = transpose_bf16(x_v[t, :])
        xT[:, t] = xt
        xf = xt.astype(F32)
        mean = jnp.sum(xf, axis=0, keepdims=True) * (1.0 / C)
        xc = xf - mean
        var = jnp.sum(xc * xc, axis=0, keepdims=True) * (1.0 / C)
        rstd = lax.rsqrt(var + EPS)
        mean_v[:, t] = mean
        rstd_v[:, t] = rstd
        u = (xc * rstd * wide(gainB) + wide(biasB)).astype(BF16)
        uT[:, t] = u
        if b == 0:
            in_w.wait()
            wT[...] = transpose_bf16(w_v[...])
        qk = nn(wT[pl.ds(0, 2 * C), :], u).astype(BF16)
        qkvT[pl.ds(0, 4), :, t] = qk.reshape(4, GC, BLK)
        qf = qk.astype(F32)
        sqr = qf * qf
        part = sqr[:, :128]
        for i in range(1, BLK // 128):
            part = part + sqr[:, 128 * i:128 * i + 128]
        ssq[...] = part if b == 0 else ssq[...] + part
        for g in range(2):
            gacc[g, :, pl.ds(0, GC)] += nt(qk[GC * g:GC * g + GC], qk[C + GC * g:C + GC * g + GC])

    sums = jnp.sum(ssq[...], axis=1, keepdims=True)
    for g in range(2):
        pack_heads(gacc, gsend, g, sums[GC * g:GC * g + GC], sums[C + GC * g:C + GC * g + GC])

    pl.semaphore_wait(barrier, 3)
    pending = []

    def send(src, dst, i, dev):
        d = remote(src, dst, i, dev)
        d.start()
        pending.append(d)
        return d

    gram_x = [send(gsend.at[core], grecv.at[1], S_GRAM + 1, cp),
              send(gsend.at[other], grecv.at[2], S_GRAM + 2, dg),
              send(gsend.at[other], grecv.at[0], S_GRAM, sib)]

    in_wo.wait()
    woT[...] = transpose_bf16(wo_v[...])
    for b in range(NB):
        t = pl.ds(b * BLK, BLK)
        if (b * BLK) % xr == 0:
            in_dy[b * BLK // xr].wait()
        v = nn(wT[pl.ds(2 * C, C), :], uT[:, t]).astype(BF16)
        qkvT[pl.ds(4, 2), :, t] = v.reshape(2, GC, BLK)
        dyt = transpose_bf16(dy_v[t, :])
        dyT[:, t] = dyt
        do = nn(wo_v[...], dyt).astype(BF16)
        doT[:, :, t] = do.reshape(2, GC, BLK)
        for g in range(2):
            dacc[g, :, pl.ds(0, GC)] += nt(do[GC * g:GC * g + GC], v[GC * g:GC * g + GC])
    for g in range(2):
        pack_heads(dacc, dsend, g)
    dprob_x = [send(dsend.at[core], drecv.at[1], S_DPROB + 1, cp),
               send(dsend.at[other], drecv.at[2], S_DPROB + 2, dg),
               send(dsend.at[other], drecv.at[0], S_DPROB, sib)]

    for d in gram_x:
        d.wait_recv()
    lane = lanes((GC, 128))
    valid = lane < HD
    head_row = rows((GC, 1))
    tcol = jnp.zeros((GC, 1), F32)
    for h in range(4):
        tcol = jnp.where((head_row >= HD * h) & (head_row < HD * h + HD), temp_ref[4 * core + h], tcol)
    gsum = unpack_heads((gsend[core] + grecv[0]) + (grecv[1] + grecv[2]))
    sq_c = col(gsum, lane, HD)
    sk_c = col(gsum, lane, HD + 1)
    nq = jnp.sqrt(sq_c)
    nk_c = jnp.sqrt(sk_c)
    nk = per_head_row(nk_c)
    den = jnp.where(valid, nq * nk, 1.0)
    cosine = jnp.where(valid, gsum / den, 0.0)
    logit = tcol * cosine
    top = jnp.max(jnp.where(valid, logit, -jnp.inf), axis=1, keepdims=True)
    e = jnp.where(valid, jnp.exp(logit - top), 0.0)
    attn = e / jnp.sum(e, axis=1, keepdims=True)
    lhsA[core] = spread_heads(attn).astype(BF16)
    attn_x = send(lhsA.at[core], lhsA.at[core], S_ATTN, sib)

    def transposed(src, dst, g):
        v = src[g]
        dst[g] = jnp.concatenate([v, jnp.zeros((64, 256), BF16)], axis=0).T[:GC]

    def reduce_send(P, R, i):
        send(P.at[sib], R.at[0], i, sib)
        send(P.at[dg], R.at[1], i + 1, sib)

    def reduce_next(P, R, T, I, i):
        remote(P.at[dg], R.at[1], i + 1, sib).wait_recv()
        T[...] = P[cp] + R[1]
        send(T, I, i + 2, cp)

    for step, g in enumerate((core, other)):
        if step == 1:
            remote(lhsA.at[other], lhsA.at[other], S_ATTN, sib).wait_recv()
        o = nn(lhsA[g][:, :GC], qkvT[4 + g])
        oT[g] = o.astype(BF16)
    Po[...] = nn(oT[...].reshape(C, NT), dy_v[...]).reshape(4, 96, C)
    reduce_send(Po, Ro, S_GWO)

    for g in range(2):
        transposed(lhsA, lhsAT, g)
        dqkvT[4 + g] = nn(lhsAT[g][:, :GC], doT[g]).astype(BF16)
    Pv[...] = nt(uT[...], dqkvT[pl.ds(4, 2)].reshape(C, NT)).reshape(4, 96, C)
    reduce_send(Pv, Rv, S_GWV)
    reduce_next(Po, Ro, To, Io, S_GWO)

    for d in dprob_x:
        d.wait_recv()
    dprob = unpack_heads((dsend[core] + drecv[0]) + (drecv[1] + drecv[2]))
    dprob = jnp.where(valid, dprob, 0.0)
    ds = attn * (dprob - jnp.sum(attn * dprob, axis=1, keepdims=True))
    dtrow = jnp.sum(ds * cosine, axis=1, keepdims=True)
    dcos = tcol * ds
    dc = dcos * cosine
    dgram = jnp.where(valid, dcos / den, 0.0)
    dsq = -0.5 * (jnp.sum(dc, axis=1, keepdims=True) / nq) / nq
    dsk = -0.5 * (per_head_sum_col(dc) / nk_c) / nk_c
    info = jnp.where(lane == 0, dsq, jnp.where(lane == 1, dsk, 0.0))
    for h in range(4):
        dt = jnp.sum(dtrow[HD * h:HD * h + HD], axis=0, keepdims=True)
        info = jnp.where((lane == 2 + h), dt, info)
    dsq_v[core] = info
    lhsD[core] = spread_heads(dgram).astype(BF16)
    send(lhsD.at[core], lhsD.at[core], S_DGRAM, sib)
    send(dsq_v.at[core], dsq_v.at[core], S_DSQ, sib)

    for step, g in enumerate((core, other)):
        if step == 1:
            remote(lhsD.at[other], lhsD.at[other], S_DGRAM, sib).wait_recv()
            remote(dsq_v.at[other], dsq_v.at[other], S_DSQ, sib).wait_recv()
        transposed(lhsD, lhsDT, g)
        dsq2 = 2.0 * dsq_v[g][:, 0:1]
        dsk2 = 2.0 * dsq_v[g][:, 1:2]
        for b in range(NB):
            t = pl.ds(b * BLK, BLK)
            q = qkvT[g, :, t]
            k = qkvT[2 + g, :, t]
            dq = nn(lhsD[g][:, :GC], k) + q.astype(F32) * dsq2
            dqkvT[g, :, t] = dq.astype(BF16)
            dk = nn(lhsDT[g][:, :GC], q) + k.astype(F32) * dsk2
            dqkvT[2 + g, :, t] = dk.astype(BF16)
    reduce_next(Pv, Rv, Tv, Iv, S_GWV)
    Pqk[...] = nt(uT[...], dqkvT[pl.ds(0, 4)].reshape(2 * C, NT)).reshape(4, 96, 2 * C)
    reduce_send(Pqk, Rqk, S_GWQK)

    outs = []
    for b in range(NB):
        t = pl.ds(b * BLK, BLK)
        o = oT[:, :, t].reshape(C, BLK)
        y = (xT[:, t].astype(F32) + nn(woT[...], o)).astype(BF16)
        outR[t, :] = transpose_bf16(y)
        if (b + 1) % 4 == 0:
            i = b // 4
            tt = pl.ds(i * 4 * BLK, 4 * BLK)
            d = local(outR.at[tt], out_hbm.at[tt], 10 + i)
            d.start()
            outs.append(d)
    reduce_next(Pqk, Rqk, Tqk, Iqk, S_GWQK)

    ggain = jnp.zeros((C, 128), F32)
    gbias = jnp.zeros((C, 128), F32)
    for b in range(NB):
        t = pl.ds(b * BLK, BLK)
        du = nn(w_v[...], dqkvT[:, :, t].reshape(3 * C, BLK))
        rstd = rstd_v[:, t]
        xhat = (xT[:, t].astype(F32) - mean_v[:, t]) * rstd
        dux = du * xhat
        pg = dux[:, :128]
        pb = du[:, :128]
        for i in range(1, BLK // 128):
            pg = pg + dux[:, 128 * i:128 * i + 128]
            pb = pb + du[:, 128 * i:128 * i + 128]
        if b == 0:
            lnacc[0] = pg
            lnacc[1] = pb
        else:
            lnacc[0] += pg
            lnacc[1] += pb
        dxh = du * wide(gainB)
        m1 = jnp.sum(dxh, axis=0, keepdims=True) * (1.0 / C)
        m2 = jnp.sum(dxh * xhat, axis=0, keepdims=True) * (1.0 / C)
        dx = rstd * (dxh - m1 - xhat * m2)
        gt = (dyT[:, t].astype(F32) + dx).astype(BF16)
        gtR[t, :] = transpose_bf16(gt)
        if (b + 1) % 4 == 0:
            i = b // 4
            tt = pl.ds(i * 4 * BLK, 4 * BLK)
            d = local(gtR.at[tt], gt_hbm.at[tt], 12 + i)
            d.start()
            outs.append(d)
    lnrow = [jnp.sum(lnacc[i].T, axis=0, keepdims=True) for i in range(2)]
    lnsend[...] = jnp.concatenate(lnrow + [jnp.zeros((6, C), F32)], axis=0)
    ln_x = [send(lnsend, lnrecv.at[0], S_LN, sib),
            send(lnsend, lnrecv.at[1], S_LN + 1, cp),
            send(lnsend, lnrecv.at[2], S_LN + 2, dg)]

    row8 = rows((8, 128))
    tl = jnp.zeros((1, 128), F32)
    l1 = lanes((1, 128))
    for g in range(2):
        for h in range(4):
            tl = jnp.where(l1 == 4 * g + h, dsq_v[g, pl.ds(0, 1), 2 + h:3 + h], tl)
    gtemp_ref[...] = tl[:, :8]

    def finish(P, R, I, i):
        remote(P.at[sib], R.at[0], i, sib).wait_recv()
        remote(I, I, i + 2, cp).wait_recv()
        return (P[s] + R[0]) + I[...]

    To2 = finish(Po, Ro, Io, S_GWO)
    Ro[0] = To2
    d = local(Ro.at[0], gwout_hbm, 14)
    d.start()
    outs.append(d)
    Rv[0] = finish(Pv, Rv, Iv, S_GWV)
    d = local(Rv.at[0], gwqkv_hbm.at[:, pl.ds(2 * C, C)], 15)
    d.start()
    outs.append(d)
    for d in ln_x:
        d.wait_recv()
    ln = (lnsend[...] + lnrecv[0]) + (lnrecv[1] + lnrecv[2])
    gg_ref[...] = ln[0:1]
    gb_ref[...] = ln[1:2]
    Rqk[0] = finish(Pqk, Rqk, Iqk, S_GWQK)
    d = local(Rqk.at[0], gwqkv_hbm.at[:, pl.ds(0, 2 * C)], 16)
    d.start()
    outs.append(d)
    for d in pending:
        d.wait_send()
    for d in outs:
        d.wait()


def scratch():
    def v(shape, dtype=F32):
        return pltpu.VMEM(shape, dtype)
    return [
        v((NT, C), BF16), v((NT, C), BF16), v((C, 3 * C), BF16), v((C, C), BF16),
        v((3 * C, C), BF16), v((C, C), BF16),
        v((C, NT), BF16), v((C, NT), BF16), v((C, NT), BF16),
        v((1, NT)), v((1, NT)),
        v((6, GC, NT), BF16), v((2, GC, NT), BF16), v((2, GC, NT), BF16),
        v((6, GC, NT), BF16), v((NT, C), BF16), v((NT, C), BF16),
        v((C, 128)), v((C, 128)), v((2 * C, 128)),
        v((2, GC, 256)), v((2, GC, 256)),
        v((2, 96, 128)), v((3, 96, 128)), v((2, 96, 128)), v((3, 96, 128)),
        v((2, GC, 256), BF16), v((2, GC, 256), BF16), v((2, GC, 256), BF16), v((2, GC, 256), BF16),
        v((2, GC, 128)),
        v((4, 96, C)), v((4, 96, C)), v((4, 96, 2 * C)),
        v((2, 96, C)), v((2, 96, C)), v((2, 96, 2 * C)),
        v((96, C)), v((96, C)), v((96, 2 * C)),
        v((96, C)), v((96, C)), v((96, 2 * C)),
        v((8, C)), v((3, 8, C)), v((2, C, 128)),
        pltpu.SemaphoreType.DMA((N_SEM,)), pltpu.SemaphoreType.DMA((N_SEM,)), pltpu.SemaphoreType.DMA((17,)),
    ]


def solution(mesh):
    row_spec = P(('dp', 'sp'), None)
    part_spec = P('dp')
    full_spec = P()

    def local_step(x_loc, dy_loc, ln_gain, ln_bias, w_qkv, w_out, temperature):
        any_spec = pl.BlockSpec(memory_space=pl.ANY)
        vmem = pl.BlockSpec(memory_space=pltpu.VMEM)
        out = pl.pallas_call(
            body,
            out_shape=(jax.ShapeDtypeStruct((NT, C), BF16), jax.ShapeDtypeStruct((NT, C), BF16),
                       jax.ShapeDtypeStruct((96, 3 * C), F32), jax.ShapeDtypeStruct((96, C), F32),
                       jax.ShapeDtypeStruct((1, C), F32), jax.ShapeDtypeStruct((1, C), F32),
                       jax.ShapeDtypeStruct((1, 8), F32)),
            in_specs=[any_spec, any_spec, vmem, vmem, any_spec, any_spec,
                      pl.BlockSpec(memory_space=pltpu.SMEM)],
            out_specs=(any_spec, any_spec, any_spec, any_spec, vmem, vmem, vmem),
            scratch_shapes=scratch(),
            compiler_params=pltpu.CompilerParams(collective_id=0, has_side_effects=True,
                                                 vmem_limit_bytes=60 * 1024 * 1024),
            name="xca",
        )(x_loc, dy_loc, ln_gain.reshape(1, C), ln_bias.reshape(1, C), w_qkv, w_out, temperature)
        return (out[0], out[1], out[2], out[3], out[4].reshape(C), out[5].reshape(C), out[6].reshape(8))

    return jax.shard_map(local_step, mesh=mesh,
                         in_specs=(row_spec, row_spec, full_spec, full_spec, full_spec, full_spec, full_spec),
                         out_specs=(row_spec, row_spec, row_spec, row_spec, part_spec, part_spec, part_spec),
                         check_vma=False)
```

```python
import jax
import jax.numpy as jnp
from jax import lax
from jax.experimental import pallas as pl
from jax.experimental.pallas import tpu as pltpu
from jax.sharding import PartitionSpec as P

F32 = jnp.float32
BF16 = jnp.bfloat16
MESH = pl.DeviceIdType.MESH
C = 384
GC = 192
HD = 48
NT = 2048
BLK = 256
NB = NT // BLK
EPS = 1e-6

S_GRAM, S_DPROB, S_ATTN, S_DGRAM, S_DSQ = 0, 3, 6, 7, 8
S_GWO, S_GWV, S_GWQK, S_LN = 9, 12, 15, 18
N_SEM = 21


def nn(a, b):
    return jnp.dot(a, b, preferred_element_type=F32)


def nt(a, b):
    return lax.dot_general(a, b, (((1,), (1,)), ((), ())), preferred_element_type=F32)


def transpose_bf16(a):
    return a.T


def lanes(shape):
    return lax.broadcasted_iota(jnp.int32, shape, len(shape) - 1)


def rows(shape):
    return lax.broadcasted_iota(jnp.int32, shape, 0)


def pack_heads(dense_ref, dst_ref, g, sq_col=None, sk_col=None):
    lane = lanes((HD, 128))
    for pair in range(2):
        total = jnp.zeros((HD, 128), F32)
        for side in range(2):
            h = 2 * pair + side
            r = pl.ds(HD * h, HD)
            block = dense_ref[g, r, :]
            block = pltpu.roll(block, (64 * side - HD * h) % 256, 1)[:, :128]
            base = 64 * side
            total = jnp.where((lane >= base) & (lane < base + HD), block, total)
            if sq_col is not None:
                rr = slice(HD * h, HD * h + HD)
                total = jnp.where(lane == base + HD, sq_col[rr], total)
                total = jnp.where(lane == base + HD + 1, sk_col[rr], total)
        dst_ref[g, pl.ds(HD * pair, HD), :] = total


def unpack_heads(packed):
    parts = []
    for pair in range(2):
        p = packed[HD * pair:HD * pair + HD]
        parts += [p, pltpu.roll(p, 64, 1)]
    return jnp.concatenate(parts, axis=0)


def spread_heads(compact):
    parts = []
    for h in range(4):
        block = compact[HD * h:HD * h + HD]
        block = jnp.concatenate([block, jnp.zeros((HD, 128), F32)], axis=1)
        parts.append(pltpu.roll(block, HD * h, 1) if h else block)
    return jnp.concatenate(parts, axis=0)


def col(x, lane, index):
    return jnp.sum(jnp.where(lane == index, x, 0.0), axis=1, keepdims=True)


def per_head_row(column):
    parts = []
    for h in range(4):
        part = jnp.broadcast_to(column[HD * h:HD * h + HD], (HD, 128))
        eye = rows((HD, 128)) == lanes((HD, 128))
        row = jnp.sum(jnp.where(eye, part, 0.0), axis=0, keepdims=True)
        parts.append(jnp.broadcast_to(row, (HD, 128)))
    return jnp.concatenate(parts, axis=0)


def per_head_sum_col(x):
    parts = []
    for h in range(4):
        row = jnp.sum(x[HD * h:HD * h + HD], axis=0, keepdims=True)
        eye = rows((HD, 128)) == lanes((HD, 128))
        parts.append(jnp.sum(jnp.where(eye, jnp.broadcast_to(row, (HD, 128)), 0.0), axis=1, keepdims=True))
    return jnp.concatenate(parts, axis=0)


def body(x_hbm, dy_hbm, gain_hbm, bias_hbm, wqkv_hbm, wout_hbm, temp_hbm,
         outR, gtR, gwqkv_o, gwout_o, small_o,
         x_v, dy_v, w_v, wo_v, wT, woT, xT, dyT, uT, mean_v, rstd_v, qkvT, doT, oT, dqkvT,
         gainB, biasB, ssq, gacc, dacc, gsend, grecv, dsend, drecv, lhsA, lhsAT, lhsD, lhsDT, dsq_v,
         Po, Pv, Pqk, Ro, Rv, Rqk, To, Tv, Tqk, Io, Iv, Iqk, lnsend, lnrecv, lnacc,
         gain_ref, bias_ref, temp_ref, ssem, rsem, dsem):
    s = lax.axis_index("sp")
    chip, core = s // 2, s % 2
    sib = chip * 2 + (1 - core)
    cp = (1 - chip) * 2 + core
    dg = (1 - chip) * 2 + (1 - core)
    other = 1 - core

    barrier = pltpu.get_barrier_semaphore()
    for dev in (sib, cp, dg):
        pl.semaphore_signal(barrier, inc=1, device_id={"sp": dev}, device_id_type=MESH)

    def remote(src, dst, i, dev):
        return pltpu.make_async_remote_copy(src_ref=src, dst_ref=dst, send_sem=ssem.at[i], recv_sem=rsem.at[i],
                                            device_id={"sp": dev}, device_id_type=MESH)

    def local(src, dst, i):
        return pltpu.make_async_copy(src, dst, dsem.at[i])

    nx = 4
    xr = NT // nx
    in_w = local(wqkv_hbm, w_v, 0)
    in_wo = local(wout_hbm, wo_v, 1)
    in_x = [local(x_hbm.at[pl.ds(i * xr, xr)], x_v.at[pl.ds(i * xr, xr)], 2 + i) for i in range(nx)]
    in_dy = [local(dy_hbm.at[pl.ds(i * xr, xr)], dy_v.at[pl.ds(i * xr, xr)], 6 + i) for i in range(nx)]
    in_small = [local(gain_hbm, gain_ref, 10), local(bias_hbm, bias_ref, 11), local(temp_hbm, temp_ref, 12)]
    in_x[0].start()
    in_small[0].start()
    in_small[1].start()
    in_w.start()
    in_small[2].start()
    for d in in_x[1:] + [in_wo] + in_dy:
        d.start()

    in_small[0].wait()
    in_small[1].wait()
    gainB[...] = jnp.broadcast_to(gain_ref[...].reshape(1, C), (128, C)).T
    biasB[...] = jnp.broadcast_to(bias_ref[...].reshape(1, C), (128, C)).T
    gacc[...] = jnp.zeros(gacc.shape, F32)
    dacc[...] = jnp.zeros(dacc.shape, F32)

    def wide(ref):
        v = ref[...]
        return jnp.concatenate([v] * (BLK // 128), axis=1)

    for b in range(NB):
        t = pl.ds(b * BLK, BLK)
        if (b * BLK) % xr == 0:
            in_x[b * BLK // xr].wait()
        xt = transpose_bf16(x_v[t, :])
        xT[:, t] = xt
        xf = xt.astype(F32)
        mean = jnp.sum(xf, axis=0, keepdims=True) * (1.0 / C)
        xc = xf - mean
        var = jnp.sum(xc * xc, axis=0, keepdims=True) * (1.0 / C)
        rstd = lax.rsqrt(var + EPS)
        mean_v[:, t] = mean
        rstd_v[:, t] = rstd
        u = (xc * rstd * wide(gainB) + wide(biasB)).astype(BF16)
        uT[:, t] = u
        if b == 0:
            in_w.wait()
            wT[...] = transpose_bf16(w_v[...])
        qk = nn(wT[pl.ds(0, 2 * C), :], u).astype(BF16)
        qkvT[pl.ds(0, 4), :, t] = qk.reshape(4, GC, BLK)
        qf = qk.astype(F32)
        sqr = qf * qf
        part = sqr[:, :128]
        for i in range(1, BLK // 128):
            part = part + sqr[:, 128 * i:128 * i + 128]
        ssq[...] = part if b == 0 else ssq[...] + part
        for g in range(2):
            gacc[g, :, pl.ds(0, GC)] += nt(qk[GC * g:GC * g + GC], qk[C + GC * g:C + GC * g + GC])

    sums = jnp.sum(ssq[...], axis=1, keepdims=True)
    for g in range(2):
        pack_heads(gacc, gsend, g, sums[GC * g:GC * g + GC], sums[C + GC * g:C + GC * g + GC])

    pl.semaphore_wait(barrier, 3)
    pending = []

    def send(src, dst, i, dev):
        d = remote(src, dst, i, dev)
        d.start()
        pending.append(d)
        return d

    gram_x = [send(gsend.at[core], grecv.at[1], S_GRAM + 1, cp),
              send(gsend.at[other], grecv.at[2], S_GRAM + 2, dg),
              send(gsend.at[other], grecv.at[0], S_GRAM, sib)]

    in_wo.wait()
    woT[...] = transpose_bf16(wo_v[...])
    for b in range(NB):
        t = pl.ds(b * BLK, BLK)
        if (b * BLK) % xr == 0:
            in_dy[b * BLK // xr].wait()
        v = nn(wT[pl.ds(2 * C, C), :], uT[:, t]).astype(BF16)
        qkvT[pl.ds(4, 2), :, t] = v.reshape(2, GC, BLK)
        dyt = transpose_bf16(dy_v[t, :])
        dyT[:, t] = dyt
        do = nn(wo_v[...], dyt).astype(BF16)
        doT[:, :, t] = do.reshape(2, GC, BLK)
        for g in range(2):
            dacc[g, :, pl.ds(0, GC)] += nt(do[GC * g:GC * g + GC], v[GC * g:GC * g + GC])
    for g in range(2):
        pack_heads(dacc, dsend, g)
    dprob_x = [send(dsend.at[core], drecv.at[1], S_DPROB + 1, cp),
               send(dsend.at[other], drecv.at[2], S_DPROB + 2, dg),
               send(dsend.at[other], drecv.at[0], S_DPROB, sib)]

    in_small[2].wait()
    for d in gram_x:
        d.wait_recv()
    lane = lanes((GC, 128))
    valid = lane < HD
    head_row = rows((GC, 1))
    tcol = jnp.zeros((GC, 1), F32)
    for h in range(4):
        tcol = jnp.where((head_row >= HD * h) & (head_row < HD * h + HD), temp_ref[4 * core + h], tcol)
    gsum = unpack_heads((gsend[core] + grecv[0]) + (grecv[1] + grecv[2]))
    sq_c = col(gsum, lane, HD)
    sk_c = col(gsum, lane, HD + 1)
    nq = jnp.sqrt(sq_c)
    nk_c = jnp.sqrt(sk_c)
    nk = per_head_row(nk_c)
    den = jnp.where(valid, nq * nk, 1.0)
    cosine = jnp.where(valid, gsum / den, 0.0)
    logit = tcol * cosine
    top = jnp.max(jnp.where(valid, logit, -jnp.inf), axis=1, keepdims=True)
    e = jnp.where(valid, jnp.exp(logit - top), 0.0)
    attn = e / jnp.sum(e, axis=1, keepdims=True)
    lhsA[core] = spread_heads(attn).astype(BF16)
    attn_x = send(lhsA.at[core], lhsA.at[core], S_ATTN, sib)

    def transposed(src, dst, g):
        v = src[g]
        dst[g] = jnp.concatenate([v, jnp.zeros((64, 256), BF16)], axis=0).T[:GC]

    def reduce_send(P, R, i):
        send(P.at[sib], R.at[0], i, sib)
        send(P.at[dg], R.at[1], i + 1, sib)

    def reduce_next(P, R, T, I, i):
        remote(P.at[dg], R.at[1], i + 1, sib).wait_recv()
        T[...] = P[cp] + R[1]
        send(T, I, i + 2, cp)

    for step, g in enumerate((core, other)):
        if step == 1:
            remote(lhsA.at[other], lhsA.at[other], S_ATTN, sib).wait_recv()
        o = nn(lhsA[g][:, :GC], qkvT[4 + g])
        oT[g] = o.astype(BF16)
    Po[...] = nn(oT[...].reshape(C, NT), dy_v[...]).reshape(4, 96, C)
    reduce_send(Po, Ro, S_GWO)

    for g in range(2):
        transposed(lhsA, lhsAT, g)
        dqkvT[4 + g] = nn(lhsAT[g][:, :GC], doT[g]).astype(BF16)
    Pv[...] = nt(uT[...], dqkvT[pl.ds(4, 2)].reshape(C, NT)).reshape(4, 96, C)
    reduce_send(Pv, Rv, S_GWV)
    reduce_next(Po, Ro, To, Io, S_GWO)

    for d in dprob_x:
        d.wait_recv()
    dprob = unpack_heads((dsend[core] + drecv[0]) + (drecv[1] + drecv[2]))
    dprob = jnp.where(valid, dprob, 0.0)
    ds = attn * (dprob - jnp.sum(attn * dprob, axis=1, keepdims=True))
    dtrow = jnp.sum(ds * cosine, axis=1, keepdims=True)
    dcos = tcol * ds
    dc = dcos * cosine
    dgram = jnp.where(valid, dcos / den, 0.0)
    dsq = -0.5 * (jnp.sum(dc, axis=1, keepdims=True) / nq) / nq
    dsk = -0.5 * (per_head_sum_col(dc) / nk_c) / nk_c
    info = jnp.where(lane == 0, dsq, jnp.where(lane == 1, dsk, 0.0))
    for h in range(4):
        dt = jnp.sum(dtrow[HD * h:HD * h + HD], axis=0, keepdims=True)
        info = jnp.where((lane == 2 + h), dt, info)
    dsq_v[core] = info
    lhsD[core] = spread_heads(dgram).astype(BF16)
    send(lhsD.at[core], lhsD.at[core], S_DGRAM, sib)
    send(dsq_v.at[core], dsq_v.at[core], S_DSQ, sib)

    for step, g in enumerate((core, other)):
        if step == 1:
            remote(lhsD.at[other], lhsD.at[other], S_DGRAM, sib).wait_recv()
            remote(dsq_v.at[other], dsq_v.at[other], S_DSQ, sib).wait_recv()
        transposed(lhsD, lhsDT, g)
        dsq2 = 2.0 * dsq_v[g][:, 0:1]
        dsk2 = 2.0 * dsq_v[g][:, 1:2]
        for b in range(NB):
            t = pl.ds(b * BLK, BLK)
            q = qkvT[g, :, t]
            k = qkvT[2 + g, :, t]
            dq = nn(lhsD[g][:, :GC], k) + q.astype(F32) * dsq2
            dqkvT[g, :, t] = dq.astype(BF16)
            dk = nn(lhsDT[g][:, :GC], q) + k.astype(F32) * dsk2
            dqkvT[2 + g, :, t] = dk.astype(BF16)
    reduce_next(Pv, Rv, Tv, Iv, S_GWV)
    Pqk[...] = nt(uT[...], dqkvT[pl.ds(0, 4)].reshape(2 * C, NT)).reshape(4, 96, 2 * C)
    reduce_send(Pqk, Rqk, S_GWQK)

    for b in range(NB):
        t = pl.ds(b * BLK, BLK)
        o = oT[:, :, t].reshape(C, BLK)
        y = (xT[:, t].astype(F32) + nn(woT[...], o)).astype(BF16)
        outR[t, :] = transpose_bf16(y)
    reduce_next(Pqk, Rqk, Tqk, Iqk, S_GWQK)

    ggain = jnp.zeros((C, 128), F32)
    gbias = jnp.zeros((C, 128), F32)
    for b in range(NB):
        t = pl.ds(b * BLK, BLK)
        du = nn(w_v[...], dqkvT[:, :, t].reshape(3 * C, BLK))
        rstd = rstd_v[:, t]
        xhat = (xT[:, t].astype(F32) - mean_v[:, t]) * rstd
        dux = du * xhat
        pg = dux[:, :128]
        pb = du[:, :128]
        for i in range(1, BLK // 128):
            pg = pg + dux[:, 128 * i:128 * i + 128]
            pb = pb + du[:, 128 * i:128 * i + 128]
        if b == 0:
            lnacc[0] = pg
            lnacc[1] = pb
        else:
            lnacc[0] += pg
            lnacc[1] += pb
        dxh = du * wide(gainB)
        m1 = jnp.sum(dxh, axis=0, keepdims=True) * (1.0 / C)
        m2 = jnp.sum(dxh * xhat, axis=0, keepdims=True) * (1.0 / C)
        dx = rstd * (dxh - m1 - xhat * m2)
        gt = (dyT[:, t].astype(F32) + dx).astype(BF16)
        gtR[t, :] = transpose_bf16(gt)
    lnrow = [jnp.sum(lnacc[i].T, axis=0, keepdims=True) for i in range(2)]
    lnsend[...] = jnp.concatenate(lnrow + [jnp.zeros((6, C), F32)], axis=0)
    ln_x = [send(lnsend, lnrecv.at[0], S_LN, sib),
            send(lnsend, lnrecv.at[1], S_LN + 1, cp),
            send(lnsend, lnrecv.at[2], S_LN + 2, dg)]

    row8 = rows((8, 128))
    tl = jnp.zeros((1, 128), F32)
    l1 = lanes((1, 128))
    for g in range(2):
        for h in range(4):
            tl = jnp.where(l1 == 4 * g + h, dsq_v[g, pl.ds(0, 1), 2 + h:3 + h], tl)
    small_o[pl.ds(2, 1), pl.ds(0, 128)] = tl

    def finish(P, R, I, i):
        remote(P.at[sib], R.at[0], i, sib).wait_recv()
        remote(I, I, i + 2, cp).wait_recv()
        return (P[s] + R[0]) + I[...]

    gwout_o[...] = finish(Po, Ro, Io, S_GWO)
    gwqkv_o[:, pl.ds(2 * C, C)] = finish(Pv, Rv, Iv, S_GWV)
    for d in ln_x:
        d.wait_recv()
    small_o[pl.ds(0, 2), :] = ((lnsend[...] + lnrecv[0]) + (lnrecv[1] + lnrecv[2]))[0:2]
    gwqkv_o[:, pl.ds(0, 2 * C)] = finish(Pqk, Rqk, Iqk, S_GWQK)
    for d in pending:
        d.wait_send()


def emit(out_v, gt_v, gwqkv_v, gwout_v, small_v, out_hbm, gt_hbm, gwqkv_hbm, gwout_hbm, gg_ref, gb_ref, gtemp_ref, sem):
    copies = [pltpu.make_async_copy(a, b, sem.at[i]) for i, (a, b) in enumerate(
        ((out_v, out_hbm), (gt_v, gt_hbm), (gwqkv_v, gwqkv_hbm), (gwout_v, gwout_hbm)))]
    for c in copies:
        c.start()
    gg_ref[...] = small_v[0, :]
    gb_ref[...] = small_v[1, :]
    gtemp_ref[...] = small_v[2, :8]
    for c in copies:
        c.wait()


def scratch():
    def v(shape, dtype=F32):
        return pltpu.VMEM(shape, dtype)
    return [
        v((NT, C), BF16), v((NT, C), BF16), v((C, 3 * C), BF16), v((C, C), BF16),
        v((3 * C, C), BF16), v((C, C), BF16),
        v((C, NT), BF16), v((C, NT), BF16), v((C, NT), BF16),
        v((1, NT)), v((1, NT)),
        v((6, GC, NT), BF16), v((2, GC, NT), BF16), v((2, GC, NT), BF16),
        v((6, GC, NT), BF16),
        v((C, 128)), v((C, 128)), v((2 * C, 128)),
        v((2, GC, 256)), v((2, GC, 256)),
        v((2, 96, 128)), v((3, 96, 128)), v((2, 96, 128)), v((3, 96, 128)),
        v((2, GC, 256), BF16), v((2, GC, 256), BF16), v((2, GC, 256), BF16), v((2, GC, 256), BF16),
        v((2, GC, 128)),
        v((4, 96, C)), v((4, 96, C)), v((4, 96, 2 * C)),
        v((2, 96, C)), v((2, 96, C)), v((2, 96, 2 * C)),
        v((96, C)), v((96, C)), v((96, 2 * C)),
        v((96, C)), v((96, C)), v((96, 2 * C)),
        v((8, C)), v((3, 8, C)), v((2, C, 128)),
        v((C,)), v((C,)), pltpu.SMEM((8,), F32),
        pltpu.SemaphoreType.DMA((N_SEM,)), pltpu.SemaphoreType.DMA((N_SEM,)), pltpu.SemaphoreType.DMA((13,)),
    ]


def solution(mesh):
    row_spec = P(('dp', 'sp'), None)
    part_spec = P('dp')
    full_spec = P()

    def local_step(x_loc, dy_loc, ln_gain, ln_bias, w_qkv, w_out, temperature):
        hbm = pl.BlockSpec(memory_space=pltpu.HBM)
        vmem = pl.BlockSpec(memory_space=pltpu.VMEM)
        args = [pltpu.with_memory_space_constraint(a, pltpu.HBM)
                for a in (x_loc, dy_loc, ln_gain, ln_bias, w_qkv, w_out, temperature)]
        out = pl.pallas_call(
            body,
            out_shape=(pltpu.VMEM((NT, C), BF16), pltpu.VMEM((NT, C), BF16), pltpu.VMEM((96, 3 * C), F32),
                       pltpu.VMEM((96, C), F32), pltpu.VMEM((8, C), F32)),
            in_specs=[hbm] * 7,
            out_specs=(vmem,) * 5,
            scratch_shapes=scratch(),
            compiler_params=pltpu.CompilerParams(collective_id=0, has_side_effects=True,
                                                 vmem_limit_bytes=48 * 1024 * 1024),
            name="xca",
        )(*args)
        out = [pltpu.with_memory_space_constraint(o, pltpu.VMEM) for o in out]
        return pl.pallas_call(
            emit,
            out_shape=(jax.ShapeDtypeStruct((NT, C), BF16), jax.ShapeDtypeStruct((NT, C), BF16),
                       jax.ShapeDtypeStruct((96, 3 * C), F32), jax.ShapeDtypeStruct((96, C), F32),
                       jax.ShapeDtypeStruct((C,), F32), jax.ShapeDtypeStruct((C,), F32),
                       jax.ShapeDtypeStruct((8,), F32)),
            in_specs=[vmem] * 5,
            out_specs=(hbm,) * 4 + (vmem,) * 3,
            scratch_shapes=[pltpu.SemaphoreType.DMA((4,))],
            compiler_params=pltpu.CompilerParams(vmem_limit_bytes=12 * 1024 * 1024),
            name="emit",
        )(*out)

    return jax.shard_map(local_step, mesh=mesh,
                         in_specs=(row_spec, row_spec, full_spec, full_spec, full_spec, full_spec, full_spec),
                         out_specs=(row_spec, row_spec, row_spec, row_spec, part_spec, part_spec, part_spec),
                         check_vma=False)
```
